128 devices in a mesh: freq: 16 (over z, x_lo, core), mode: 8 (over x_hi, y).
Axes of the slice: x: 4 (x_hi: 2, x_lo: 2; x = x_hi * 2 + x_lo), y: 4, z: 4, core: 2. Of those that a mesh axis runs over, the one named last changes fastest.
Arguments:
- sources: bfloat16 [32, 512, 2, 4096], P(None, None, None, ('freq', 'mode')), may hold values from -6 to 6
- mapping: bfloat16 [32, 2, 2048, 4096], P('freq', None, 'mode'), may hold values from -0.0625 to 0.0625
Outputs:
- pressure: bfloat16 [32, 512, 2, 2048], P(None, 'freq', None, 'mode')
The draws below stay inside these ranges and needn't reach their ends.
All inputs are finite; a program needn't handle non-finite values.
Results may differ from the reference program's by a relative error of at most 0.0006.
Values may be sent and summed in bfloat16 or wider, within the bound.
No kernel may reach another device: no remote copies, remote signals or barrier semaphores. Data moves between devices by JAX's collectives and lax.ppermute only.
A program may use at most 128 MiB of HBM per device.

```python
import jax
import jax.numpy as jnp
from jax import lax

MODES = 4096
OBS = 2048
SNAP = 512
BINS = 32


def shard_levels(rng, shape, split, smallest, high):
    def one(dim, blocks):
        draws = jax.random.uniform(jax.random.fold_in(jax.random.fold_in(rng, 6), dim), (blocks,), jnp.float32, smallest / len(split), high / len(split))
        return jnp.repeat(jnp.exp(draws), shape[dim] // blocks).reshape((-1,) + (1,) * (len(shape) - dim - 1))

    loudness = one(*split[0])
    for cut in split[1:]:
        loudness = loudness * one(*cut)
    return loudness


def noise(rng, shape, width, reach, pieces=(), held_as=jnp.bfloat16):
    drawn = jax.random.normal(rng, shape, jnp.float32) * width
    if len(pieces) > 0:
        drawn = shard_levels(rng, shape, pieces, -0.22, 0.18) * drawn
    return jnp.clip(drawn, min=-reach, max=reach).astype(held_as)


def setup_inputs(seed: int = 0) -> dict:
    arg_keys = jax.random.split(jax.random.key(seed), 3)
    sources = noise(arg_keys[0], (BINS, SNAP, 2, MODES), 1.0, 6.0, ((3, 128),))
    mapping = noise(arg_keys[1], (BINS, 2, OBS, MODES), (2 * MODES) ** -0.5, 0.0625, ((0, 16), (2, 8)))
    return {"sources": sources, "mapping": mapping}


def map_bin(arrays):
    spectra, matrix = arrays
    spectra = spectra.astype(jnp.float32)
    matrix = matrix.astype(jnp.float32)
    high = lax.Precision.HIGHEST
    real_part = jnp.einsum('sm,om->so', spectra[:, 0], matrix[0], precision=high) - jnp.einsum('sm,om->so', spectra[:, 1], matrix[1], precision=high)
    imag_part = jnp.einsum('sm,om->so', spectra[:, 1], matrix[0], precision=high) + jnp.einsum('sm,om->so', spectra[:, 0], matrix[1], precision=high)
    return jnp.stack([real_part, imag_part], axis=1)

def reference(sources, mapping):
    field = lax.map(map_bin, (sources, mapping))
    weights = ((jnp.arange(BINS, dtype=jnp.float32) + 1.0) / BINS) ** 2
    energy = jnp.sum(weights[:, None, None, None] * field * field) / (SNAP * OBS)
    factor = jnp.sqrt(BINS / (energy + 1e-06))
    return (field * factor).astype(jnp.bfloat16)
```

```python
import jax
import jax.numpy as jnp
from jax import lax
from jax.experimental import pallas as pl
from jax.experimental.pallas import tpu as pltpu
from jax.sharding import Mesh
from jax.sharding import PartitionSpec as P

FREQ = ("freq_0", "freq_1", "freq_2")
MODE = ("mode_0", "mode_1")
AXES = ("freq_0", "freq_1", "freq_2", "mode_0", "mode_1")
BF16 = jnp.bfloat16
F32 = jnp.float32


def linear(z, x, c, y):
    return (((z % 4 * 2 + x % 2) * 2 + c % 2) * 2 + x % 4 // 2) * 4 + y % 4


def hop(value, target):
    pairs = [
        (linear(z, x, c, y), linear(*target(z, x, c, y)))
        for z in range(4)
        for x in range(4)
        for c in range(2)
        for y in range(4)
    ]
    return lax.ppermute(value, AXES, pairs)


def vmem_call(kernel, out_shapes, where, *arrays, flops=0, moved=None):
    outs = [jax.ShapeDtypeStruct(s, d) for s, d in out_shapes]
    if moved is None:
        moved = sum(a.size * a.dtype.itemsize for a in arrays) * 2
    return pl.pallas_call(
        kernel,
        out_shape=outs,
        grid_spec=pltpu.PrefetchScalarGridSpec(
            num_scalar_prefetch=1,
            grid=(1,),
            in_specs=[whole(a.shape) for a in arrays],
            out_specs=[whole(s) for s, _ in out_shapes],
        ),
        cost_estimate=pl.CostEstimate(flops=max(flops, moved), bytes_accessed=moved, transcendentals=0),
    )(where, *arrays)


def whole(shape):
    return pl.BlockSpec(shape, lambda g, w: (0,) * len(shape))


def pack_kernel(where, t_ref, *outs):
    z, xl, c, y = where[0], where[1], where[2], where[4]
    for crel in range(2):
        for dz in range(4):
            zt = (z + dz) % 4
            for i in range(4):
                k = (zt + 1 + i) % 4
                lanes = pl.ds(pl.multiple_of(k * 128, 128), 128)
                for brel in range(2):
                    for xrel in range(2):
                        block = t_ref[zt, xl ^ xrel, c ^ crel, (y % 2) ^ brel, :, :, lanes]
                        if i == 0:
                            outs[crel * 4 + dz][brel, xrel] = block
                        else:
                            outs[8 + crel * 4 + dz][i - 1, brel, xrel] = block


def join_y_kernel(part, where, *refs):
    pieces, (same, other) = refs[:8], refs[8:]
    for s in range(8):
        for xrel in range(2):
            if part is None:
                same[xrel, s] = pieces[s][0, xrel]
                other[xrel, s] = pieces[s][1, xrel]
            else:
                same[xrel, s] = pieces[s][part, 0, xrel]
                other[xrel, s] = pieces[s][part, 1, xrel]


def join_x_kernel(where, *refs):
    pieces, (same, other) = refs[:4], refs[4:]
    for s in range(4):
        same[s] = pieces[s][0]
        other[s] = pieces[s][1]


ROWS = 128


def field_kernel(where, s0, s2, sm, sp, own, near_r, near_i, out, energy, full):
    z, xl, c, xh, y = where[0], where[1], where[2], where[3], where[4]
    g = pl.program_id(0)

    @pl.when(g == 0)
    def _():
        x = xh * 2 + xl
        for dx, piece in ((0, s0), (2, s2), (3, sm), (1, sp)):
            xs = (x + dx) % 4
            for yi, dy in enumerate((0, 2, 3, 1)):
                ys = (y + dy) % 4
                for crel in range(2):
                    for dz in range(4):
                        zs = (z + 4 - dz) % 4
                        row = zs * 1024 + (xs % 2) * 512 + (c ^ crel) * 256 + (xs // 2) * 128 + ys * 32
                        rows = pl.ds(pl.multiple_of(row, 32), 32)
                        full[rows, 0:128] = piece[yi, crel * 4 + dz, 0]
                        full[rows, 128:256] = piece[yi, crel * 4 + dz, 1]
        energy[...] = jnp.zeros_like(energy)

    total = jnp.zeros((8, 128), F32)
    spectra = full[...]
    for o in range(2):
        if o == 0:
            left_r, left_i = own[0, 0], own[0, 1]
        else:
            left_r, left_i = near_r[...], near_i[...]
        with_r = jnp.dot(left_r, spectra, preferred_element_type=F32)
        with_i = jnp.dot(left_i, spectra, preferred_element_type=F32)
        real = with_r[:, :128] - with_i[:, 128:]
        imag = with_r[:, 128:] + with_i[:, :128]
        square = real * real + imag * imag
        total = total + jnp.sum(square.reshape(ROWS // 8, 8, 128), axis=0)
        real_t, imag_t = real.T, imag.T
        for q in range(4):
            d = (xl * 2 + c) ^ q
            out[o, d, 0] = real_t[q * 32 : q * 32 + 32]
            out[o, d, 1] = imag_t[q * 32 : q * 32 + 32]
    energy[...] += total


def field_call(where, pieces, mapping, near_r, near_i):
    piece = whole(pieces[0].shape)
    return pl.pallas_call(
        field_kernel,
        out_shape=[
            jax.ShapeDtypeStruct((2, 4, 2, 32, 256), F32),
            jax.ShapeDtypeStruct((8, 128), F32),
        ],
        grid_spec=pltpu.PrefetchScalarGridSpec(
            num_scalar_prefetch=1,
            grid=(256 // ROWS,),
            in_specs=[piece] * 4
            + [
                pl.BlockSpec((1, 2, ROWS, 4096), lambda g, w: (w[4] % 2, 0, g, 0)),
                pl.BlockSpec((ROWS, 4096), lambda g, w: (g, 0)),
                pl.BlockSpec((ROWS, 4096), lambda g, w: (g, 0)),
            ],
            out_specs=[
                pl.BlockSpec((2, 4, 2, 32, ROWS), lambda g, w: (0, 0, 0, 0, g)),
                pl.BlockSpec((8, 128), lambda g, w: (0, 0)),
            ],
            scratch_shapes=[pltpu.VMEM((4096, 256), BF16)],
        ),
        cost_estimate=pl.CostEstimate(flops=2 * 1024 * 4096 * 256, bytes_accessed=11 << 20, transcendentals=0),
        compiler_params=pltpu.CompilerParams(vmem_limit_bytes=48 << 20),
    )(where, *pieces, mapping, near_r, near_i)


def split_kernel(where, *refs):
    fields, outs = refs[:4], refs[4:]
    for o in range(2):
        for d in range(4):
            for i in range(4):
                outs[o * 4 + d][i] = fields[i][o, d]


def last_kernel(where, factor, *refs):
    parts, out = refs[:8], refs[8]
    z, xl, c, y = where[0], where[1], where[2], where[4]
    for o in range(2):
        for d in range(4):
            for i in range(4):
                zs = (z + 3 - i) % 4
                xls, cs = xl ^ (d // 2), c ^ (d % 2)
                row = zs * 8 + xls * 4 + cs * 2 + ((y + o) % 2)
                scaled = (parts[o * 4 + d][i] * factor[0, 0]).astype(BF16)
                out[row, :, 0:256] = scaled[0]
                out[row, :, 256:512] = scaled[1]


def body(sources, mapping):
    where = jnp.stack([lax.axis_index(a) for a in AXES]).astype(jnp.int32)
    c, y = where[2], where[4]
    kept = y % 2
    table = jnp.transpose(sources, (0, 2, 3, 1)).reshape(4, 2, 2, 2, 2, 32, 512)
    first = (2, 2, 2, 32, 128)
    packed = vmem_call(
        pack_kernel, [(first, BF16)] * 8 + [((3,) + first, BF16)] * 8, where, table
    )

    def exchange(blocks):
        got = [blocks[0]]
        for n in range(1, 8):
            crel, dz = n // 4, n % 4
            got.append(hop(blocks[n], lambda z, x, c, y: (z + dz, x, c + crel, y)))
        return got

    early = exchange(packed[:8])
    late = exchange(packed[8:])

    def move_mapping(part):
        rows = lax.dynamic_slice(mapping, (1 - kept, part, 0, 0), (1, 1, 256, 4096))[0, 0]
        return hop(rows, lambda z, x, c, y: (z, x, c, y + (1 if c else 3)))

    near = [move_mapping(0), move_mapping(1)]

    fields, energies = [], []
    yshape = (2, 8, 2, 32, 128)
    xshape = (4, 8, 2, 32, 128)
    for i in range(4):
        pieces = early if i == 0 else late
        part = None if i == 0 else i - 1
        same, other = vmem_call(
            lambda *r, part=part: join_y_kernel(part, *r),
            [(yshape, BF16)] * 2,
            where,
            *pieces,
            moved=1 << 20,
        )
        y2 = hop(same, lambda z, x, c, y: (z, x, c, y + 2))
        yp = hop(other, lambda z, x, c, y: (z, x, c, y + 1))
        ym = hop(other, lambda z, x, c, y: (z, x, c, y + 3))
        same, other = vmem_call(join_x_kernel, [(xshape, BF16)] * 2, where, same, y2, yp, ym)
        x2 = hop(same, lambda z, x, c, y: (z, x + 2, c, y))
        xp = hop(other, lambda z, x, c, y: (z, x + 1, c, y))
        xm = hop(other, lambda z, x, c, y: (z, x + 3, c, y))
        field, energy = field_call(where, (same, x2, xp, xm), mapping, *near)
        energies.append(energy)
        if i < 3:
            field = hop(field, lambda z, x, c, y: (z + 1 + i, x, c, y))
        fields.append(field)

    freq = (where[0] * 2 + where[1]) * 2 + where[2]
    weight = ((freq * 2 + kept + 1).astype(F32) / 32) ** 2
    local_energy = jnp.sum(energies[0] + energies[1] + energies[2] + energies[3]) * weight
    shared = lax.all_to_all(
        jnp.broadcast_to(local_energy, (128, 1)), AXES, split_axis=0, concat_axis=0, tiled=True
    )
    energy = jnp.sum(shared) / (512 * 2048)
    factor = jnp.sqrt(32 / (energy + 1e-06))

    parts = vmem_call(split_kernel, [((4, 2, 32, 256), F32)] * 8, where, *fields)
    landed = [parts[0]]
    for n in range(1, 8):
        o, xrel, crel = n // 4, n // 2 % 2, n % 2
        landed.append(
            hop(
                parts[n],
                lambda z, x, c, y: (
                    z,
                    x ^ xrel,
                    c ^ crel,
                    y + (o if c == 0 else -o),
                ),
            )
        )
    result = vmem_call(last_kernel, [((32, 32, 512), BF16)], where, factor.reshape(1, 1), *landed)[0]
    return result.reshape(32, 32, 2, 256)


def solution(mesh):
    torus = Mesh(mesh.devices.reshape(4, 2, 2, 2, 4), AXES)
    return jax.shard_map(
        body,
        mesh=torus,
        in_specs=(P(None, None, None, AXES), P(FREQ, None, MODE, None)),
        out_specs=P(None, FREQ, None, MODE),
        check_vma=False,
    )
```

```python
import jax
import jax.numpy as jnp
from jax import lax
from jax.experimental import pallas as pl
from jax.experimental.pallas import tpu as pltpu
from jax.sharding import Mesh
from jax.sharding import PartitionSpec as P


FREQ = ("freq_0", "freq_1", "freq_2")
MODE = ("mode_0", "mode_1")
AXES = ("freq_0", "freq_1", "freq_2", "mode_0", "mode_1")
BF16 = jnp.bfloat16
F32 = jnp.float32


def linear(z, x, c, y):
    return (((z % 4 * 2 + x % 2) * 2 + c % 2) * 2 + x % 4 // 2) * 4 + y % 4


def hop(value, target):
    pairs = [
        (linear(z, x, c, y), linear(*target(z, x, c, y)))
        for z in range(4)
        for x in range(4)
        for c in range(2)
        for y in range(4)
    ]
    return lax.ppermute(value, AXES, pairs)


def vmem_call(kernel, out_shapes, where, *arrays):
    outs = [jax.ShapeDtypeStruct(s, d) for s, d in out_shapes]
    moved = sum(a.size * a.dtype.itemsize for a in arrays) * 2
    return pl.pallas_call(
        kernel,
        out_shape=outs,
        grid_spec=pltpu.PrefetchScalarGridSpec(
            num_scalar_prefetch=1,
            grid=(1,),
            in_specs=[whole(a.shape) for a in arrays],
            out_specs=[whole(s) for s, _ in out_shapes],
        ),
        cost_estimate=pl.CostEstimate(flops=moved, bytes_accessed=moved, transcendentals=0),
    )(where, *arrays)


def whole(shape):
    return pl.BlockSpec(shape, lambda g, w: (0,) * len(shape))


def pack_early_kernel(where, t_ref, *outs):
    z, xl, c, y = where[0], where[1], where[2], where[4]
    for peer in range(8):
        zt, ct = (z + peer % 4) % 4, c ^ (peer // 4)
        for i in range(2):
            lanes = pl.ds(pl.multiple_of((zt + 1 + i) % 4 * 128, 128), 128)
            for brel in range(2):
                for xrel in range(2):
                    outs[peer][i, brel, xrel] = t_ref[
                        zt, xl ^ xrel, ct, (y % 2) ^ brel, :, :, lanes
                    ]


def pack_late_kernel(where, t_ref, out):
    xl, y = where[1], where[4]
    for peer in range(8):
        zt, ct = peer // 2, peer % 2
        for i in range(2):
            k = (zt + 3 + i) % 4
            for brel in range(2):
                for xrel in range(2):
                    out[peer, i, brel, xrel] = t_ref[
                        zt, xl ^ xrel, ct, (y % 2) ^ brel, :, :, k * 128 : k * 128 + 128
                    ]


def join_early_kernel(where, *refs):
    pieces, outs = refs[:8], refs[8:]
    z, c = where[0], where[2]
    for peer in range(8):
        s = (z + 4 - peer % 4) % 4 * 2 + (c ^ (peer // 4))
        for part in range(2):
            for xrel in range(2):
                outs[part * 2][xrel, s] = pieces[peer][part, 0, xrel]
                outs[part * 2 + 1][xrel, s] = pieces[peer][part, 1, xrel]


def join_late_kernel(where, pieces, *outs):
    for part in range(2):
        for s in range(8):
            for xrel in range(2):
                outs[part * 2][xrel, s] = pieces[s, part, 0, xrel]
                outs[part * 2 + 1][xrel, s] = pieces[s, part, 1, xrel]


def join_x_kernel(where, *refs):
    pieces, (same, other) = refs[:4], refs[4:]
    for s in range(4):
        same[s] = pieces[s][0]
        other[s] = pieces[s][1]


ROWS = 128


def order_rows(where, pieces, full):
    xl, xh, y = where[1], where[3], where[4]
    x = xh * 2 + xl
    for dx, piece in zip((0, 2, 3, 1), pieces):
        xs = (x + dx) % 4
        for yi, dy in enumerate((0, 2, 3, 1)):
            ys = (y + dy) % 4
            for s in range(8):
                row = s // 2 * 1024 + (xs % 2) * 512 + s % 2 * 256 + (xs // 2) * 128 + ys * 32
                rows = pl.ds(pl.multiple_of(row, 32), 32)
                full[rows, 0:128] = piece[yi, s, 0]
                full[rows, 128:256] = piece[yi, s, 1]


def field_kernel(closing, where, *refs):
    pieces, refs, full = refs[:4], refs[4:-1], refs[-1]
    if closing:
        before, running, refs = refs[5:8], refs[-1], refs[:5] + refs[8:-1]
    own, near_r0, near_i0, near_r1, near_i1, out, energy = refs
    if not closing:
        running = energy

    @pl.when(pl.program_id(0) == 0)
    def _():
        order_rows(where, pieces, full)
        if closing:
            running[...] = before[0][...] + before[1][...] + before[2][...]
        else:
            running[...] = jnp.zeros_like(running)

    total = jnp.zeros((8, 128), F32)
    spectra = full[...]

    def times(*lefts):
        width = 4096 // len(lefts)
        parts = [
            jnp.dot(left, spectra[n * width : n * width + width], preferred_element_type=F32)
            for n, left in enumerate(lefts)
        ]
        return sum(parts[1:], parts[0])

    for o, (with_r, with_i) in enumerate(
        (
            (times(own[0, 0]), times(own[0, 1])),
            (times(near_r0[...], near_r1[...]), times(near_i0[...], near_i1[...])),
        )
    ):
        real = with_r[:, :128] - with_i[:, 128:]
        imag = with_r[:, 128:] + with_i[:, :128]
        square = real * real + imag * imag
        total = total + jnp.sum(square.reshape(ROWS // 8, 8, 128), axis=0)
        for part, value in enumerate((real, imag)):
            value = value.T
            for q in range(4):
                out[o, q, part] = value[q * 32 : q * 32 + 32]
    running[...] += total
    if closing:
        number = ((where[0] * 2 + where[1]) * 2 + where[2]) * 2 + where[4] % 2 + 1
        weight = (number.astype(F32) / 32) ** 2
        line = jnp.sum(running[...], axis=0, keepdims=True) * weight
        energy[...] = jnp.broadcast_to(line, energy.shape)


def field_call(where, spectra, mapping, near, before=()):
    closing = len(before) > 0
    lines = (128, 128) if closing else (8, 128)
    shape = (2, 4, 2, 32, 256)
    scratch = [pltpu.VMEM((8, 128), F32)] if closing else []
    return pl.pallas_call(
        lambda *r: field_kernel(closing, *r),
        out_shape=[jax.ShapeDtypeStruct(s, F32) for s in (shape, lines)],
        grid_spec=pltpu.PrefetchScalarGridSpec(
            num_scalar_prefetch=1,
            grid=(256 // ROWS,),
            in_specs=[whole(a.shape) for a in spectra]
            + [pl.BlockSpec((1, 2, ROWS, 4096), lambda g, w: (w[4] % 2, 0, g, 0))]
            + [pl.BlockSpec((ROWS, 2048), lambda g, w: (g, 0))] * 4
            + [whole((8, 128))] * len(before),
            out_specs=[
                pl.BlockSpec((2, 4, 2, 32, ROWS), lambda g, w: (0, 0, 0, 0, g)),
                pl.BlockSpec(lines, lambda g, w: (0, 0)),
            ],
            scratch_shapes=scratch + [pltpu.VMEM((4096, 256), BF16)],
        ),
        cost_estimate=pl.CostEstimate(flops=2 * 1024 * 4096 * 256, bytes_accessed=11 << 20, transcendentals=0),
        compiler_params=pltpu.CompilerParams(vmem_limit_bytes=48 << 20),
    )(where, *spectra, mapping, *near, *before)


def take_kernel(where, rows_ref, out):
    out[...] = rows_ref[0, 0]


def take_mapping(where, mapping, part, half):
    return pl.pallas_call(
        take_kernel,
        out_shape=jax.ShapeDtypeStruct((256, 2048), BF16),
        grid_spec=pltpu.PrefetchScalarGridSpec(
            num_scalar_prefetch=1,
            grid=(2,),
            in_specs=[pl.BlockSpec((1, 1, 128, 2048), lambda g, w: (1 - w[4] % 2, part, g, half))],
            out_specs=pl.BlockSpec((128, 2048), lambda g, w: (g, 0)),
        ),
        cost_estimate=pl.CostEstimate(flops=2 << 20, bytes_accessed=2 << 20, transcendentals=0),
    )(where, mapping)


def scale_kernel(where, shared, *refs):
    fields, outs = refs[:4], refs[4:]
    energy = jnp.sum(shared[...]) / (512 * 2048)
    factor = jnp.sqrt(32 / (energy + 1e-06))
    for d in range(4):
        q = (where[1] * 2 + where[2]) ^ d
        for o in range(2):
            for i in range(4):
                outs[o * 4 + d][i] = (fields[i][o, q] * factor).astype(BF16)


def last_kernel(where, *refs):
    parts, out = refs[:8], refs[8]
    z, xl, c, y = where[0], where[1], where[2], where[4]
    for o in range(2):
        for d in range(4):
            for i in range(4):
                zs = (z + 3 - i) % 4
                row = zs * 8 + (d ^ (xl * 2 + c)) * 2 + (y + o) % 2
                out[row, :, 0, :] = parts[o * 4 + d][i, 0]
                out[row, :, 1, :] = parts[o * 4 + d][i, 1]


def return_hop(value, n):
    o, xrel, crel = n // 4, n // 2 % 2, n % 2
    return hop(value, lambda z, x, c, y: (z, x ^ xrel, c ^ crel, y + (o if c == 0 else -o)))


def return_all(parts):
    landed = {n: return_hop(parts[n], n) for n in (2, 3, 6, 7, 4, 5, 1)}
    return [parts[0]] + [landed[n] for n in range(1, 8)]


def steps(sources, mapping):
    where = jnp.stack([lax.axis_index(a) for a in AXES]).astype(jnp.int32)
    table = jnp.transpose(sources, (0, 2, 3, 1)).reshape(4, 2, 2, 2, 2, 32, 512)
    block = (2, 2, 2, 32, 128)
    blocks = vmem_call(pack_early_kernel, [((2,) + block, BF16)] * 8, where, table)
    late = vmem_call(pack_late_kernel, [((8, 2) + block, BF16)], where, table)[0]
    early = [blocks[0]]
    for n in range(1, 8):
        crel, dz = n // 4, n % 4
        early.append(hop(blocks[n], lambda z, x, c, y: (z + dz, x, c + crel, y)))
    late = lax.all_to_all(
        late, ("freq_0", "freq_2"), split_axis=0, concat_axis=0, tiled=True
    )

    near = []
    for n in range(4):
        rows = take_mapping(where, mapping, n % 2, n // 2)
        near.append(hop(rows, lambda z, x, c, y: (z, x, c, y + (1 if c else 3))))

    yshape = (2, 8, 2, 32, 128)
    xshape = (4, 8, 2, 32, 128)
    joined = vmem_call(join_early_kernel, [(yshape, BF16)] * 4, where, *early)
    joined += vmem_call(join_late_kernel, [(yshape, BF16)] * 4, where, late)

    fields, energies = [], []
    for i in range(4):
        same, other = joined[2 * i], joined[2 * i + 1]
        y2 = hop(same, lambda z, x, c, y: (z, x, c, y + 2))
        yp = hop(other, lambda z, x, c, y: (z, x, c, y + 1))
        ym = hop(other, lambda z, x, c, y: (z, x, c, y + 3))
        same, other = vmem_call(join_x_kernel, [(xshape, BF16)] * 2, where, same, y2, yp, ym)
        x2 = hop(same, lambda z, x, c, y: (z, x + 2, c, y))
        xp = hop(other, lambda z, x, c, y: (z, x + 1, c, y))
        xm = hop(other, lambda z, x, c, y: (z, x + 3, c, y))
        spectra = (same, x2, xp, xm)
        field, energy = field_call(where, spectra, mapping, near, energies if i == 3 else ())
        energies.append(energy)
        if i < 3:
            field = hop(field, lambda z, x, c, y: (z + 1 + i, x, c, y))
        fields.append(field)

    shared = lax.all_to_all(energy, AXES, split_axis=0, concat_axis=0, tiled=True)

    parts = vmem_call(
        scale_kernel, [((4, 2, 32, 256), BF16)] * 8, where, shared, *fields
    )
    landed = return_all(parts)
    return vmem_call(last_kernel, [((32, 32, 2, 256), BF16)], where, *landed)[0]


def solution(mesh):
    torus = Mesh(mesh.devices.reshape(4, 2, 2, 2, 4), AXES)
    return jax.shard_map(
        steps,
        mesh=torus,
        in_specs=(P(None, None, None, AXES), P(FREQ, None, MODE, None)),
        out_specs=P(None, FREQ, None, MODE),
        check_vma=False,
    )
```
